8 devices in a mesh: dp: 1 (over z), ch: 2 (over y), wd: 4 (over x, core).
Axes of the slice: x: 2, y: 2, z: 1, core: 2. Of those that a mesh axis runs over, the one named last changes fastest.
Arguments:
- resid_in: bfloat16 [8192, 4096], P('dp', 'wd')
- seg_pos: int32 [2, 4096], P('dp')
- gain_temporal: bfloat16 [4096], P('wd')
- w_x: bfloat16 [4096, 5632], P('wd', 'ch')
- bias_x: bfloat16 [5632], P('ch')
- w_y: bfloat16 [4096, 5632], P('wd', 'ch')
- bias_y: bfloat16 [5632], P('ch')
- conv_w: bfloat16 [4, 5632], P(None, 'ch')
- conv_bias: bfloat16 [5632], P('ch')
- lam_param: float32 [5632], P('ch')
- rgate_w: bfloat16 [22, 256, 256], P('ch')
- rgate_b: bfloat16 [5632], P('ch')
- igate_w: bfloat16 [22, 256, 256], P('ch')
- igate_b: bfloat16 [5632], P('ch')
- w_o: bfloat16 [5632, 4096], P('ch', 'wd')
- bias_o: bfloat16 [4096], P('wd')
- gain_mlp: bfloat16 [4096], P('wd')
- w_g: bfloat16 [4096, 12288], P('wd', 'ch')
- bias_g: bfloat16 [12288], P('ch')
- w_u: bfloat16 [4096, 12288], P('wd', 'ch')
- bias_u: bfloat16 [12288], P('ch')
- w_d: bfloat16 [12288, 4096], P('ch', 'wd')
- bias_d: bfloat16 [4096], P('wd')
Outputs:
- output: bfloat16 [8192, 4096], P('dp', 'wd')
All inputs are finite; a program needn't handle non-finite values.
Results may differ from the reference program's by a relative error of at most 0.0130632.
Values are sent between devices in bfloat16 or wider.
A program may use at most 1 GiB of HBM per device.

```python
import jax
import jax.numpy as jnp
from jax import lax

D = 4096
D_RNN = 5632
F = 12288
BLOCKS = 22
B = 2
T = 4096
CONV_WIDTH = 4
BLOCK_WIDTH = D_RNN // BLOCKS
EPS = 1e-6


def normal_draw(key, shape, scale):
    return (jax.random.normal(key, shape, jnp.float32) * scale).astype(jnp.bfloat16)


def doc_positions(key):
    cuts = jax.random.randint(key, (B, 4), 0, T)
    steps = jnp.arange(T, dtype=jnp.int32)
    starts = jnp.any(steps[None, :, None] == cuts[:, None, :], axis=2) | (steps == 0)[None, :]
    last_start = lax.cummax(jnp.where(starts, steps[None, :], 0), axis=1)
    return (steps[None, :] - last_start).astype(jnp.int32)


def setup_inputs(seed: int = 0, part: int = 0) -> dict:
    root = jax.random.key(seed)
    part_key = jax.random.fold_in(root, part)
    keys = jax.random.split(root, 24)
    col_ramp = 0.5 + 1.5 * jnp.arange(D, dtype=jnp.float32) / D
    noise = jax.random.normal(jax.random.fold_in(part_key, 0), (B * T, D), jnp.float32)
    decay_target = jax.random.uniform(keys[9], (D_RNN,), jnp.float32, 0.9, 0.999)
    sigma_lam = decay_target ** 0.125
    return {
        'resid_in': (noise * col_ramp).astype(jnp.bfloat16),
        'seg_pos': doc_positions(jax.random.fold_in(part_key, 1)),
        'gain_temporal': normal_draw(keys[0], (D,), 0.5),
        'w_x': normal_draw(keys[1], (D, D_RNN), D ** -0.5),
        'bias_x': normal_draw(keys[2], (D_RNN,), 0.5),
        'w_y': normal_draw(keys[3], (D, D_RNN), D ** -0.5),
        'bias_y': normal_draw(keys[4], (D_RNN,), 0.5),
        'conv_w': normal_draw(keys[5], (CONV_WIDTH, D_RNN), 0.5),
        'conv_bias': normal_draw(keys[6], (D_RNN,), 0.5),
        'lam_param': jnp.log(sigma_lam / (1.0 - sigma_lam)),
        'rgate_w': normal_draw(keys[7], (BLOCKS, BLOCK_WIDTH, BLOCK_WIDTH), BLOCK_WIDTH ** -0.5),
        'rgate_b': normal_draw(keys[8], (D_RNN,), 1.0),
        'igate_w': normal_draw(keys[10], (BLOCKS, BLOCK_WIDTH, BLOCK_WIDTH), BLOCK_WIDTH ** -0.5),
        'igate_b': normal_draw(keys[11], (D_RNN,), 1.0),
        'w_o': normal_draw(keys[12], (D_RNN, D), 1.5 * D_RNN ** -0.5),
        'bias_o': normal_draw(keys[13], (D,), 0.5),
        'gain_mlp': normal_draw(keys[14], (D,), 0.5),
        'w_g': normal_draw(keys[15], (D, F), D ** -0.5),
        'bias_g': normal_draw(keys[16], (F,), 0.5),
        'w_u': normal_draw(keys[17], (D, F), D ** -0.5),
        'bias_u': normal_draw(keys[18], (F,), 0.5),
        'w_d': normal_draw(keys[19], (F, D), 1.5 * F ** -0.5),
        'bias_d': normal_draw(keys[20], (D,), 0.5),
    }


def rms_scale(vals, gain):
    mean_sq = jnp.mean(vals * vals, axis=-1, keepdims=True)
    return (vals * lax.rsqrt(mean_sq + EPS) * (1.0 + gain.astype(jnp.float32))).astype(jnp.bfloat16)


def conv_mix(vals, positions, conv_w, conv_bias):
    vals32 = vals.astype(jnp.float32)
    taps = conv_w.astype(jnp.float32)
    total = conv_bias.astype(jnp.float32) + vals32 * taps[0]
    for shift in range(1, CONV_WIDTH):
        moved = jnp.pad(vals32[:-shift], ((shift, 0), (0, 0)))
        total = total + jnp.where((positions >= shift)[:, None], moved, 0.0) * taps[shift]
    return total.astype(jnp.bfloat16)


def combine(left, right):
    return left[0] * right[0], right[0] * left[1] + right[1]


def rg_lru(conv_out, positions, lam_param, rgate_w, rgate_b, igate_w, igate_b):
    grouped = conv_out.astype(jnp.float32).reshape(T, BLOCKS, BLOCK_WIDTH)
    rate = jax.nn.sigmoid(jnp.einsum('tbi,bij->tbj', grouped, rgate_w.astype(jnp.float32)).reshape(T, D_RNN) + rgate_b.astype(jnp.float32))
    inflow = jax.nn.sigmoid(jnp.einsum('tbi,bij->tbj', grouped, igate_w.astype(jnp.float32)).reshape(T, D_RNN) + igate_b.astype(jnp.float32))
    log_a = -8.0 * rate * jax.nn.softplus(-lam_param.astype(jnp.float32))
    reset = (positions == 0)[:, None]
    decay = jnp.where(reset, 0.0, jnp.exp(log_a))
    scale = jnp.where(reset, 1.0, jnp.sqrt(-jnp.expm1(2.0 * log_a)))
    drive = scale * inflow * conv_out.astype(jnp.float32)
    return lax.associative_scan(combine, (decay, drive), axis=0)[1]


def reference(resid_in, seg_pos, gain_temporal, w_x, bias_x, w_y, bias_y, conv_w, conv_bias, lam_param, rgate_w, rgate_b, igate_w, igate_b, w_o, bias_o, gain_mlp, w_g, bias_g, w_u, bias_u, w_d, bias_d):
    def one_sequence(pair):
        seq_x, positions = pair
        resid32 = seq_x.astype(jnp.float32)
        normed = rms_scale(resid32, gain_temporal)
        y_branch = jax.nn.gelu(jnp.dot(normed, w_y, preferred_element_type=jnp.float32) + bias_y.astype(jnp.float32), approximate=True).astype(jnp.bfloat16)
        u_branch = (jnp.dot(normed, w_x, preferred_element_type=jnp.float32) + bias_x.astype(jnp.float32)).astype(jnp.bfloat16)
        conv_out = conv_mix(u_branch, positions, conv_w, conv_bias)
        hidden = rg_lru(conv_out, positions, lam_param, rgate_w, rgate_b, igate_w, igate_b)
        mixed = (hidden * y_branch.astype(jnp.float32)).astype(jnp.bfloat16)
        resid = resid32 + jnp.dot(mixed, w_o, preferred_element_type=jnp.float32) + bias_o.astype(jnp.float32)
        normed2 = rms_scale(resid, gain_mlp)
        gate = jax.nn.gelu(jnp.dot(normed2, w_g, preferred_element_type=jnp.float32) + bias_g.astype(jnp.float32), approximate=True)
        upper = jnp.dot(normed2, w_u, preferred_element_type=jnp.float32) + bias_u.astype(jnp.float32)
        inner = (gate * upper).astype(jnp.bfloat16)
        return (resid + jnp.dot(inner, w_d, preferred_element_type=jnp.float32) + bias_d.astype(jnp.float32)).astype(jnp.bfloat16)
    per_seq = lax.map(one_sequence, (resid_in.reshape(B, T, D), seg_pos))
    return per_seq.reshape(B * T, D)
```

```python
import jax
import jax.numpy as jnp
from jax import lax
from jax.experimental import pallas as pl
from jax.experimental.pallas import tpu as pltpu
from jax.sharding import PartitionSpec as P


EPS = 1e-6
CHUNKS = 3
ROWS = 128
COLS = 512
TIME_BLOCK = 256


bf16 = jnp.bfloat16
f32 = jnp.float32


def dot(a, b):
    return jnp.dot(a, b, preferred_element_type=f32)


def recurrence_kernel(u_ref, y_ref, pos_ref, conv_w_ref, conv_b_ref, rate_ref, rw_ref, rb_ref, iw_ref, ib_ref, out_ref, ext, dec, drv, carry):
    rows, width = u_ref.shape
    groups = rows // 8

    @pl.when(pl.program_id(1) == 0)
    def _():
        ext[0:8, :] = jnp.zeros((8, width), f32)
        carry[...] = jnp.zeros_like(carry)

    pos = pos_ref[...]
    u = u_ref[...].astype(f32)
    ext[8:8 + rows, :] = u
    taps = conv_w_ref[...].astype(f32)
    total = conv_b_ref[...].astype(f32) + u * taps[0:1]
    for shift in range(1, conv_w_ref.shape[0]):
        total = total + jnp.where(pos >= shift, ext[8 - shift:8 - shift + rows, :], 0.0) * taps[shift:shift + 1]
    ext[0:8, :] = u[rows - 8:rows]
    conv = total.astype(bf16)
    rate = jax.nn.sigmoid(dot(conv, rw_ref[...]) + rb_ref[...].astype(f32))
    inflow = jax.nn.sigmoid(dot(conv, iw_ref[...]) + ib_ref[...].astype(f32))
    log_a = rate * rate_ref[...]
    decay = jnp.exp(log_a)
    scale = jnp.sqrt(-jnp.tanh(log_a) * (decay * decay + 1.0))
    reset = pos == 0
    decay = jnp.where(reset, 0.0, decay)
    scale = jnp.where(reset, 1.0, scale)
    drive = scale * inflow * conv.astype(f32)
    a = decay.reshape(groups, 8, width)
    b = drive.reshape(groups, 8, width)
    row = lax.broadcasted_iota(jnp.int32, (groups, 8, width), 1)
    for step in (1, 2, 4):
        keep = row >= step
        b = a * jnp.where(keep, pltpu.roll(b, step, 1), 0.0) + b
        a = a * jnp.where(keep, pltpu.roll(a, step, 1), 1.0)
    dec[...] = a
    drv[...] = b
    state = carry[0:1, :]
    for group in range(groups):
        hidden = dec[group] * state + drv[group]
        drv[group] = hidden
        state = hidden[7:8, :]
    carry[0:1, :] = state
    out_ref[...] = (drv[...].reshape(rows, width) * y_ref[...].astype(f32)).astype(bf16)


def recurrence(u, y, pos, conv_w, conv_b, rate, rw, rb, iw, ib):
    tokens, width = u.shape
    blocks, block = rw.shape[0], rw.shape[1]
    time_spec = pl.BlockSpec((TIME_BLOCK, block), lambda b, t: (t, b))
    row_spec = pl.BlockSpec((1, block), lambda b, t: (0, b))
    gate_spec = pl.BlockSpec((None, block, block), lambda b, t: (b, 0, 0))
    return pl.pallas_call(
        recurrence_kernel,
        grid=(blocks, tokens // TIME_BLOCK),
        in_specs=[time_spec, time_spec, pl.BlockSpec((TIME_BLOCK, 1), lambda b, t: (t, 0)),
                  pl.BlockSpec((conv_w.shape[0], block), lambda b, t: (0, b)), row_spec, row_spec,
                  gate_spec, row_spec, gate_spec, row_spec],
        out_specs=time_spec,
        out_shape=jax.ShapeDtypeStruct((tokens, width), bf16),
        scratch_shapes=[pltpu.VMEM((TIME_BLOCK + 8, block), f32), pltpu.VMEM((TIME_BLOCK // 8, 8, block), f32),
                        pltpu.VMEM((TIME_BLOCK // 8, 8, block), f32), pltpu.VMEM((8, block), f32)],
        compiler_params=pltpu.CompilerParams(dimension_semantics=("arbitrary", "arbitrary")),
        cost_estimate=pl.CostEstimate(flops=tokens * width * 1200, bytes_accessed=tokens * width * 6, transcendentals=tokens * width * 8),
        name="recurrence",
    )(u, y, pos, conv_w, conv_b[None], rate[None], rw, rb[None], iw, ib[None])


def inner_kernel(m_ref, *refs):
    gate_w, up_w, (gate_b, up_b, out_ref) = refs[:4], refs[4:8], refs[8:]
    depth = gate_w[0].shape[0]
    rows = m_ref.shape[0] // 4

    @pl.loop(0, 4)
    def _(part):
        at = pl.ds(part * rows, rows)

        def product(ws):
            return sum(dot(m_ref[at, j * depth:(j + 1) * depth], w[...]) for j, w in enumerate(ws))

        gate = jax.nn.gelu(product(gate_w) + gate_b[...].astype(f32), approximate=True)
        out_ref[at, :] = (gate * (product(up_w) + up_b[...].astype(f32))).astype(bf16)


def inner_of(m, gate_w, up_w, gate_b, up_b):
    tokens, width = m.shape
    depth, size = gate_w[0].shape
    weight = pl.BlockSpec((depth, COLS), lambda n: (0, n))
    vector = pl.BlockSpec((1, COLS), lambda n: (0, n))
    return pl.pallas_call(
        inner_kernel, grid=(size // COLS,),
        in_specs=[pl.BlockSpec((tokens, width), lambda n: (0, 0))] + [weight] * 8 + [vector] * 2,
        out_specs=pl.BlockSpec((tokens, COLS), lambda n: (0, n)),
        out_shape=jax.ShapeDtypeStruct((tokens, size), bf16),
        cost_estimate=pl.CostEstimate(flops=4 * tokens * width * size, bytes_accessed=4 * width * size + 2 * tokens * (width + size), transcendentals=tokens * size),
        name="inner")(m, *gate_w, *up_w, gate_b[None], up_b[None])


def tie(*values):
    return lax.optimization_barrier(values)


def pick(parts, quarter):
    value = parts[0][...]
    for index in range(1, 4):
        value = jnp.where(quarter == index, parts[index][...], value)
    return value.astype(f32)


def write_norm(pieces, gain_ref, out_ref):
    width = pieces[0].shape[1]
    total = sum(jnp.sum(p * p, axis=1, keepdims=True) for p in pieces)
    inv = lax.rsqrt(total / (width * len(pieces)) + EPS)
    for j, p in enumerate(pieces):
        out_ref[:, j * width:(j + 1) * width] = (p * inv * (1.0 + gain_ref[j:j + 1, :])).astype(bf16)


def norm_kernel(at_ref, own_ref, near_ref, *refs):
    far, diag, (gain_ref, out_ref) = refs[:4], refs[4:8], refs[8:]
    quarter = pl.program_id(0) // (pl.num_programs(0) // 4)
    pieces = [own_ref[...].astype(f32), near_ref[...].astype(f32), pick(far, quarter), pick(diag, quarter)]
    write_norm(pieces, gain_ref, out_ref)


def norm_in(own, near, far, diag, gain):
    tokens, width = own.shape
    rows = 2 * ROWS
    per = tokens // rows // 4
    whole = pl.BlockSpec((rows, width), lambda i, at: (i, 0))
    parts = [pl.BlockSpec((rows, width), lambda i, at, q=q: (jnp.clip(i - q * per, 0, per - 1), 0)) for q in range(4)]
    spec = pltpu.PrefetchScalarGridSpec(
        num_scalar_prefetch=1, grid=(tokens // rows,),
        in_specs=[whole, whole] + parts + parts + [pl.BlockSpec((4, width), lambda i, at: (0, 0))],
        out_specs=pl.BlockSpec((rows, 4 * width), lambda i, at: (i, 0)))
    return pl.pallas_call(
        norm_kernel, grid_spec=spec, out_shape=jax.ShapeDtypeStruct((tokens, 4 * width), bf16),
        cost_estimate=pl.CostEstimate(flops=tokens * width * 600, bytes_accessed=tokens * width * 16, transcendentals=0),
        name="norm_in")(jnp.zeros((1,), jnp.int32), own, near, *far, *diag, gain)


def resid_kernel(at_ref, own_ref, near_ref, *refs):
    far, diag, kept, got = refs[:4], refs[4:8], refs[8:12], refs[12:16]
    bias_ref, gain_ref = refs[16:18]
    out, norm_ref = refs[18:22], refs[22]
    quarter = at_ref[2]
    base = [own_ref[...].astype(f32), near_ref[...].astype(f32), pick(far, quarter), pick(diag, quarter)]
    pieces = [b + (k[...] + g[...].astype(f32)) + bias_ref[j:j + 1, :] for j, (b, k, g) in enumerate(zip(base, kept, got))]
    for o, p in zip(out, pieces):
        o[...] = p
    write_norm(pieces, gain_ref, norm_ref)


def resid_norm(at, own, near, far, diag, kept, got, bias, gain):
    tokens, width = kept[0].shape
    per = tokens // ROWS

    def at_row(k):
        return pl.BlockSpec((ROWS, width), lambda i, at: (at[k] * per + i, 0))

    whole = pl.BlockSpec((ROWS, width), lambda i, at: (i, 0))
    parts = [pl.BlockSpec((ROWS, width), lambda i, at, q=q: (jnp.where(at[2] == q, i, 0), 0)) for q in range(4)]
    vector = pl.BlockSpec((4, width), lambda i, at: (0, 0))
    spec = pltpu.PrefetchScalarGridSpec(
        num_scalar_prefetch=1, grid=(per,),
        in_specs=[at_row(0), at_row(1)] + parts + parts + [whole] * 8 + [vector] * 2,
        out_specs=[whole] * 4 + [pl.BlockSpec((ROWS, 4 * width), lambda i, at: (i, 0))])
    shape = jax.ShapeDtypeStruct((tokens, width), f32)
    out = pl.pallas_call(
        resid_kernel, grid_spec=spec, out_shape=[shape] * 4 + [jax.ShapeDtypeStruct((tokens, 4 * width), bf16)],
        cost_estimate=pl.CostEstimate(flops=tokens * width * 1600, bytes_accessed=tokens * width * 40, transcendentals=0),
        name="resid_norm")(at, own, near, *far, *diag, *kept, *got, bias, gain)
    return out[:4], out[4]


def solution(mesh):
    row_spec = P('dp', 'wd')
    specs = (row_spec, P('dp', None), P('wd'), P('wd', 'ch'), P('ch'), P('wd', 'ch'), P('ch'), P(None, 'ch'), P('ch'), P('ch'), P('ch', None, None), P('ch'), P('ch', None, None), P('ch'), P('ch', 'wd'), P('wd'), P('wd'), P('wd', 'ch'), P('ch'), P('wd', 'ch'), P('ch'), P('ch', 'wd'), P('wd'))

    def pc(a):
        return lax.ppermute(a, 'wd', [(i, i ^ 1) for i in range(4)])

    def over_x(a, flip):
        return lax.ppermute(a, 'wd', [(i, i ^ flip) for i in range(4)])

    def px(a):
        return over_x(a, 2)

    def pd(a):
        return over_x(a, 3)

    def py(a):
        return lax.ppermute(a, 'ch', [(0, 1), (1, 0)])

    def local_layer(resid_in, seg_pos, gain_temporal, w_x, bias_x, w_y, bias_y, conv_w, conv_bias, lam_param, rgate_w, rgate_b, igate_w, igate_b, w_o, bias_o, gain_mlp, w_g, bias_g, w_u, bias_u, w_d, bias_d):
        tokens, local_width = resid_in.shape
        _, steps = seg_pos.shape
        half, quarter = steps // 2, steps // 4
        wd = lax.axis_index('wd')
        cy = lax.axis_index('ch')
        cx, core = wd // 2, wd % 2
        blocks, block = rgate_w.shape[0], rgate_w.shape[1]
        my_blocks = (blocks + 1) // 2
        first_block = core * (blocks - my_blocks)
        other_block = (1 - core) * (blocks - my_blocks)
        lanes = my_blocks * block

        def rows(a, start, size):
            return lax.dynamic_slice_in_dim(a, start, size, axis=0)

        def cols(a, start, size):
            return lax.dynamic_slice_in_dim(a, start, size, axis=a.ndim - 1)

        def my_cols(w):
            return cols(w, first_block * block, lanes)

        x_first = [rows(resid_in, (1 - cx) * steps + cy * half + c * quarter, quarter) for c in range(2)]
        far_mine = [px(a) for a in x_first]
        vec = jnp.stack([gain_temporal, gain_mlp, bias_o, bias_d])
        vecs = [vec, pc(vec), px(vec), pd(vec)]
        x_own = rows(resid_in, cx * steps, steps)
        x_near = pc(x_own)
        shares = []
        for w in (w_y, w_x):
            mine, others = my_cols(w), cols(w, other_block * block, lanes)
            shares.append((mine, pc(others), px(mine), pd(others)))
        wo_far = px(w_o)
        size = w_g.shape[1] // CHUNKS
        parts = [slice(c * size, (c + 1) * size) for c in range(CHUNKS)]
        mlp = []
        for part in parts:
            ws = (w_g[:, part], w_u[:, part], w_d[part])
            mlp.append([(w, pc(w), px(w)) for w in ws])

        table = jnp.stack([v.astype(f32) for v in vecs], axis=1)
        gain_t, gain_m, b_o, b_d = table[0], table[1], table[2], table[3]

        far_other = [py(a) for a in far_mine]
        low = cy == 0

        def quarters(mine, other):
            return [jnp.where(low, m, o) for m, o in zip(mine, other)] + [jnp.where(low, o, m) for m, o in zip(mine, other)]

        far = quarters(far_mine, far_other)
        diag = quarters([pc(a) for a in far_mine], [pc(a) for a in far_other])
        normed = norm_in(x_own, x_near, far, diag, gain_t)

        wy_all = jnp.concatenate(shares[0], axis=0)
        y = jax.nn.gelu(dot(normed, wy_all) + my_cols(bias_y).astype(f32), approximate=True).astype(bf16)
        y, *wx = tie(y, *shares[1])
        u = (dot(normed, jnp.concatenate(wx, axis=0)) + my_cols(bias_x).astype(f32)).astype(bf16)
        rate = -8.0 * jax.nn.softplus(-my_cols(lam_param))
        pos = rows(seg_pos, cx, 1).reshape(steps, 1)
        mixed = recurrence(u, y, pos, my_cols(conv_w), my_cols(conv_bias), rate,
                           rows(rgate_w, first_block, my_blocks), my_cols(rgate_b),
                           rows(igate_w, first_block, my_blocks), my_cols(igate_b))
        mixed, wo_far = tie(mixed, wo_far)

        kept = rows(mixed, core * half, half)
        got = pc(rows(mixed, (1 - core) * half, half))
        first = core == 0
        mixed_all = jnp.concatenate([jnp.where(first, kept, got), jnp.where(first, got, kept)[:, 2 * lanes - blocks * block:]], axis=1)
        wo = [w_o, pc(w_o), wo_far, pc(wo_far)]
        mixed_send = rows(mixed_all, (1 - cy) * quarter, quarter)
        mixed_keep = rows(mixed_all, cy * quarter, quarter)
        received = [py(dot(mixed_send, w).astype(bf16)) for w in wo]
        own = [dot(mixed_keep, w) for w in wo]
        my_quarter = core * 2 + cy
        at = jnp.stack([cx * 4 + my_quarter, my_quarter, my_quarter]).astype(jnp.int32)
        resid, m_own = resid_norm(at, resid_in, x_near, far, diag, own, received, b_o, gain_m)
        m_other = py(m_own)
        m = [m_own, m_other]

        acc = [[None] * 4, [None] * 4]

        def relay(w, far_piece):
            return [w[0], w[1], far_piece, pc(far_piece)]

        def up(s, c, gate_w, up_w):
            return inner_of(m[s], gate_w, up_w, bias_g[parts[c]], bias_u[parts[c]])

        def add_down(s, inner, d_all):
            for j in (3, 2, 1, 0):
                term = dot(inner, d_all[j])
                acc[s][j] = term if acc[s][j] is None else acc[s][j] + term

        def after(s, *extra):
            flat = tie(*acc[s], *extra)
            acc[s] = list(flat[:4])
            return flat[4:]

        (g0, u0, d0), (g1, u1, d1), (g2, u2, d2) = mlp
        m[0], far_g, far_u = tie(m[0], g0[2], u0[2])
        g0, u0 = relay(g0, far_g), relay(u0, far_u)
        inner, far_d = tie(up(0, 0, g0, u0), d0[2])
        d0 = relay(d0, far_d)
        add_down(0, inner, d0)
        far_g, far_u = after(0, g1[2], u1[2])
        g1, u1 = relay(g1, far_g), relay(u1, far_u)
        inner_own, m[1] = tie(up(0, 1, g1, u1), m[1])
        inner, inner_own, far_d = tie(up(1, 0, g0, u0), inner_own, d1[2])
        d1 = relay(d1, far_d)
        add_down(1, inner, d0)
        m[1], = after(1, m[1])
        inner = up(1, 1, g1, u1)
        inner, inner_own = tie(inner, inner_own)
        add_down(0, inner_own, d1)
        add_down(1, inner, d1)
        flat = tie(*acc[0], *acc[1], g2[2], u2[2])
        acc = [list(flat[:4]), list(flat[4:8])]
        g2, u2 = relay(g2, flat[8]), relay(u2, flat[9])
        inner = [up(0, 2, g2, u2), up(1, 2, g2, u2)]
        inner[0], inner[1], far_d = tie(inner[0], inner[1], d2[2])
        d2 = relay(d2, far_d)
        add_down(1, inner[1], d2)
        add_down(0, inner[0], d2)

        down = [None] * 4
        for j in (3, 2, 1, 0):
            down[j] = py(acc[1][j].astype(bf16))
        pieces = []
        for j in (3, 2, 1, 0):
            out = (resid[j] + (acc[0][j] + down[j].astype(f32)) + b_d[j]).astype(bf16)
            moved = out if j == 0 else (pc, lambda a: over_x(a, 2), lambda a: over_x(a, 3))[j - 1](out)
            pieces.append((j, moved, py(moved)))
        result = jnp.zeros((tokens, local_width), bf16)
        for j, mine, other in pieces:
            base = jnp.bitwise_xor(wd, j) * half
            result = lax.dynamic_update_slice_in_dim(result, mine, base + cy * quarter, axis=0)
            result = lax.dynamic_update_slice_in_dim(result, other, base + (1 - cy) * quarter, axis=0)
        return result

    return jax.shard_map(local_layer, mesh=mesh, in_specs=specs, out_specs=row_spec, check_vma=False)
```

```python
import jax
import jax.numpy as jnp
from jax import lax
from jax.experimental import pallas as pl
from jax.experimental.pallas import tpu as pltpu
from jax.sharding import PartitionSpec as P


EPS = 1e-6
CHUNKS = (2560, 1024, 1024, 1024, 512)
ROWS = 128
COLS = 512
SPLIT = 768
TIME_BLOCK = 256


bf16 = jnp.bfloat16
f32 = jnp.float32


def dot(a, b):
    return jnp.dot(a, b, preferred_element_type=f32)


def recurrence_kernel(u_ref, pos_ref, conv_w_ref, conv_b_ref, rate_ref, rw_ref, rb_ref, iw_ref, ib_ref, out_ref, ext, dec, drv, carry):
    rows, width = u_ref.shape
    groups = rows // 8

    @pl.when(pl.program_id(1) == 0)
    def _():
        ext[0:8, :] = jnp.zeros((8, width), f32)
        carry[...] = jnp.zeros_like(carry)

    pos = pos_ref[...]
    u = u_ref[...].astype(f32)
    ext[8:8 + rows, :] = u
    taps = conv_w_ref[...].astype(f32)
    total = conv_b_ref[...].astype(f32) + u * taps[0:1]
    for shift in range(1, conv_w_ref.shape[0]):
        total = total + jnp.where(pos >= shift, ext[8 - shift:8 - shift + rows, :], 0.0) * taps[shift:shift + 1]
    ext[0:8, :] = u[rows - 8:rows]
    conv = total.astype(bf16)
    rate = jax.nn.sigmoid(dot(conv, rw_ref[...]) + rb_ref[...].astype(f32))
    inflow = jax.nn.sigmoid(dot(conv, iw_ref[...]) + ib_ref[...].astype(f32))
    log_a = rate * rate_ref[...]
    decay = jnp.exp(log_a)
    scale = jnp.sqrt(-jnp.tanh(log_a) * (decay * decay + 1.0))
    reset = pos == 0
    decay = jnp.where(reset, 0.0, decay)
    scale = jnp.where(reset, 1.0, scale)
    drive = scale * inflow * conv.astype(f32)
    a = decay.reshape(groups, 8, width)
    b = drive.reshape(groups, 8, width)
    row = lax.broadcasted_iota(jnp.int32, (groups, 8, width), 1)
    for step in (1, 2, 4):
        keep = row >= step
        b = a * jnp.where(keep, pltpu.roll(b, step, 1), 0.0) + b
        a = a * jnp.where(keep, pltpu.roll(a, step, 1), 1.0)
    dec[...] = a
    drv[...] = b
    state = carry[0:1, :]
    for group in range(groups):
        hidden = dec[group] * state + drv[group]
        drv[group] = hidden
        state = hidden[7:8, :]
    carry[0:1, :] = state
    out_ref[...] = drv[...].reshape(rows, width)


def recurrence(u, pos, conv_w, conv_b, rate, rw, rb, iw, ib):
    tokens, width = u.shape
    blocks, block = rw.shape[0], rw.shape[1]
    time_spec = pl.BlockSpec((TIME_BLOCK, block), lambda b, t: (t, b))
    row_spec = pl.BlockSpec((1, block), lambda b, t: (0, b))
    gate_spec = pl.BlockSpec((None, block, block), lambda b, t: (b, 0, 0))
    return pl.pallas_call(
        recurrence_kernel,
        grid=(blocks, tokens // TIME_BLOCK),
        in_specs=[time_spec, pl.BlockSpec((TIME_BLOCK, 1), lambda b, t: (t, 0)),
                  pl.BlockSpec((conv_w.shape[0], block), lambda b, t: (0, b)), row_spec, row_spec,
                  gate_spec, row_spec, gate_spec, row_spec],
        out_specs=time_spec,
        out_shape=jax.ShapeDtypeStruct((tokens, width), f32),
        scratch_shapes=[pltpu.VMEM((TIME_BLOCK + 8, block), f32), pltpu.VMEM((TIME_BLOCK // 8, 8, block), f32),
                        pltpu.VMEM((TIME_BLOCK // 8, 8, block), f32), pltpu.VMEM((8, block), f32)],
        compiler_params=pltpu.CompilerParams(dimension_semantics=("arbitrary", "arbitrary")),
        cost_estimate=pl.CostEstimate(flops=tokens * width * 1200, bytes_accessed=tokens * width * 6, transcendentals=tokens * width * 8),
        name="recurrence",
    )(u, pos, conv_w, conv_b[None], rate[None], rw, rb[None], iw, ib[None])


def products(x, ws):
    depth = ws[0].shape[0]
    return sum(dot(x[:, j * depth:(j + 1) * depth], w[...]) for j, w in enumerate(ws))


def inner_kernel(low_ref, high_ref, *refs):
    gate_w, up_w, gate_b, up_b, out_ref = refs[:4], refs[4:8], refs[8], refs[9], refs[-1]
    rows = low_ref.shape[0]
    for part, m_ref in enumerate((low_ref, high_ref)):
        gate = jax.nn.gelu(products(m_ref, gate_w) + gate_b[...].astype(f32), approximate=True)
        out_ref[part * rows:(part + 1) * rows, :] = (gate * (products(m_ref, up_w) + up_b[...].astype(f32))).astype(bf16)


def inner_of(m, gate_w, up_w, gate_b, up_b, first, total, into=None):
    rows, width = m[0].shape
    depth, size = gate_w[0].shape
    tokens = 2 * rows
    weight = pl.BlockSpec((depth, COLS), lambda n: (0, n))
    vector = pl.BlockSpec((1, COLS), lambda n: (0, n))
    offset = first // COLS
    given = [] if into is None else [into]
    return pl.pallas_call(
        inner_kernel, grid=(size // COLS,),
        in_specs=[pl.BlockSpec((rows, width), lambda n: (0, 0))] * 2 + [weight] * 8 + [vector] * 2 + [pl.BlockSpec(memory_space=pl.ANY)] * len(given),
        out_specs=pl.BlockSpec((tokens, COLS), lambda n: (0, offset + n)),
        out_shape=jax.ShapeDtypeStruct((tokens, total), bf16),
        input_output_aliases={12: 0} if given else {},
        cost_estimate=pl.CostEstimate(flops=4 * tokens * width * size, bytes_accessed=4 * width * size + 2 * tokens * (width + size), transcendentals=tokens * size),
        name="inner")(*m, *gate_w, *up_w, gate_b[None], up_b[None], *given)


def project_kernel(at_ref, n_ref, *refs):
    ws, bias_ref, out_ref = refs[:4], refs[4], refs[-1]
    out_ref[...] = (products(n_ref, ws) + bias_ref[...].astype(f32)).astype(bf16)


def mix_kernel(at_ref, n_ref, *refs):
    ws, bias_ref, hidden_ref, out_ref = refs[:4], refs[4], refs[5], refs[-1]
    y = jax.nn.gelu(products(n_ref, ws) + bias_ref[...].astype(f32), approximate=True).astype(bf16)
    out_ref[...] = (hidden_ref[...] * y.astype(f32)).astype(bf16)


def project(normed, ws, bias, start, tokens, hidden=None):
    width = normed.shape[1]
    depth, size = ws[0].shape
    rows = 1024
    per = tokens // rows
    tile = pl.BlockSpec((rows, COLS), lambda i, n, at: (at[0] * per + i, n))
    given = [] if hidden is None else [hidden]
    spec = pltpu.PrefetchScalarGridSpec(
        num_scalar_prefetch=1, grid=(per, size // COLS),
        in_specs=[pl.BlockSpec((rows, width), lambda i, n, at: (at[0] * per + i, 0))] + [pl.BlockSpec((depth, COLS), lambda i, n, at: (0, n))] * 4
        + [pl.BlockSpec((1, COLS), lambda i, n, at: (0, n))] + [tile] * len(given),
        out_specs=pl.BlockSpec((rows, COLS), lambda i, n, at: (i, n)))
    return pl.pallas_call(
        project_kernel if hidden is None else mix_kernel, grid_spec=spec, out_shape=jax.ShapeDtypeStruct((tokens, size), bf16),
        cost_estimate=pl.CostEstimate(flops=2 * tokens * width * size, bytes_accessed=2 * (tokens + size) * width, transcendentals=tokens * size),
        name="project")(jnp.asarray(start, jnp.int32).reshape(1), normed, *ws, bias[None], *given)


def tie(*values):
    return lax.optimization_barrier(values)


def pick(parts, quarter):
    value = parts[0][...]
    for index in range(1, 4):
        value = jnp.where(quarter == index, parts[index][...], value)
    return value.astype(f32)


def write_norm(pieces, gain_ref, out_ref):
    width = pieces[0].shape[1]
    total = sum(jnp.sum(p * p, axis=1, keepdims=True) for p in pieces)
    inv = lax.rsqrt(total / (width * len(pieces)) + EPS)
    for j, p in enumerate(pieces):
        out_ref[:, j * width:(j + 1) * width] = (p * inv * (1.0 + gain_ref[j:j + 1, :])).astype(bf16)


def norm_kernel(at_ref, own_ref, near_ref, *refs):
    far, diag, (gain_ref, out_ref) = refs[:4], refs[4:8], refs[8:]
    quarter = (pl.program_id(0) // (pl.num_programs(0) // 4) + at_ref[0]) % 4
    pieces = [own_ref[...].astype(f32), near_ref[...].astype(f32), pick(far, quarter), pick(diag, quarter)]
    write_norm(pieces, gain_ref, out_ref)


def norm_in(shift, own, near, far, diag, gain):
    tokens, width = own.shape
    rows = 2 * ROWS
    per = tokens // rows // 4
    whole = pl.BlockSpec((rows, width), lambda i, at: (i, 0))
    parts = [pl.BlockSpec((rows, width), lambda i, at, q=q: (jnp.clip(i - (q + at[0]) % 4 * per, 0, per - 1), 0)) for q in range(4)]
    spec = pltpu.PrefetchScalarGridSpec(
        num_scalar_prefetch=1, grid=(tokens // rows,),
        in_specs=[whole, whole] + parts + parts + [pl.BlockSpec((4, width), lambda i, at: (0, 0))],
        out_specs=pl.BlockSpec((rows, 4 * width), lambda i, at: (i, 0)))
    return pl.pallas_call(
        norm_kernel, grid_spec=spec, out_shape=jax.ShapeDtypeStruct((tokens, 4 * width), bf16),
        cost_estimate=pl.CostEstimate(flops=tokens * width * 600, bytes_accessed=tokens * width * 16, transcendentals=0),
        name="norm_in")(shift, own, near, *far, *diag, gain)


def resid_kernel(at_ref, own_ref, near_ref, *refs):
    far, diag, kept, got = refs[:4], refs[4:8], refs[8:12], refs[12:16]
    bias_ref, gain_ref = refs[16:18]
    out, norm_ref = refs[-5:-1], refs[-1]
    quarter = at_ref[2]
    base = [own_ref[...].astype(f32), near_ref[...].astype(f32), pick(far, quarter), pick(diag, quarter)]
    pieces = [b + (k[...] + g[...].astype(f32)) + bias_ref[j:j + 1, :] for j, (b, k, g) in enumerate(zip(base, kept, got))]
    for o, p in zip(out, pieces):
        o[...] = p
    write_norm(pieces, gain_ref, norm_ref)


def resid_norm(at, part, own, near, far, diag, kept, got, bias, gain, into=()):
    rows, width = got[0].shape
    tokens = kept[0].shape[0]
    all_blocks, per = tokens // ROWS, rows // ROWS
    base = part * per

    def at_row(k):
        return pl.BlockSpec((ROWS, width), lambda i, at: (at[k] * all_blocks + base + i, 0))

    here = pl.BlockSpec((ROWS, width), lambda i, at: (base + i, 0))
    whole = pl.BlockSpec((ROWS, width), lambda i, at: (i, 0))
    parts = [pl.BlockSpec((ROWS, width), lambda i, at, q=q: (jnp.where(at[2] == q, base + i, 0), 0)) for q in range(4)]
    vector = pl.BlockSpec((4, width), lambda i, at: (0, 0))
    spec = pltpu.PrefetchScalarGridSpec(
        num_scalar_prefetch=1, grid=(per,),
        in_specs=[at_row(0), at_row(1)] + parts + parts + [here] * 4 + [whole] * 4 + [vector] * 2 + [pl.BlockSpec(memory_space=pl.ANY)] * len(into),
        out_specs=[here] * 4 + [pl.BlockSpec((ROWS, 4 * width), lambda i, at: (i, 0))])
    shape = jax.ShapeDtypeStruct((tokens, width), f32)
    out = pl.pallas_call(
        resid_kernel, grid_spec=spec, out_shape=[shape] * 4 + [jax.ShapeDtypeStruct((rows, 4 * width), bf16)],
        input_output_aliases={21 + j: j for j in range(len(into))},
        cost_estimate=pl.CostEstimate(flops=rows * width * 1600, bytes_accessed=rows * width * 40, transcendentals=0),
        name="resid_norm")(at, own, near, *far, *diag, *kept, *got, bias, gain, *into)
    return out[:4], out[4]


def solution(mesh):
    row_spec = P('dp', 'wd')
    specs = (row_spec, P('dp', None), P('wd'), P('wd', 'ch'), P('ch'), P('wd', 'ch'), P('ch'), P(None, 'ch'), P('ch'), P('ch'), P('ch', None, None), P('ch'), P('ch', None, None), P('ch'), P('ch', 'wd'), P('wd'), P('wd'), P('wd', 'ch'), P('ch'), P('wd', 'ch'), P('ch'), P('ch', 'wd'), P('wd'))

    def pc(a):
        return lax.ppermute(a, 'wd', [(i, i ^ 1) for i in range(4)])

    def over_x(a, flip):
        return lax.ppermute(a, 'wd', [(i, i ^ flip) for i in range(4)])

    def px(a):
        return over_x(a, 2)

    def pd(a):
        return over_x(a, 3)

    def py(a):
        return lax.ppermute(a, 'ch', [(0, 1), (1, 0)])

    def local_layer(resid_in, seg_pos, gain_temporal, w_x, bias_x, w_y, bias_y, conv_w, conv_bias, lam_param, rgate_w, rgate_b, igate_w, igate_b, w_o, bias_o, gain_mlp, w_g, bias_g, w_u, bias_u, w_d, bias_d):
        tokens, local_width = resid_in.shape
        _, steps = seg_pos.shape
        half, quarter = steps // 2, steps // 4
        wd = lax.axis_index('wd')
        cy = lax.axis_index('ch')
        cx, core = wd // 2, wd % 2
        blocks, block = rgate_w.shape[0], rgate_w.shape[1]
        my_blocks = (blocks + 1) // 2
        first_block = core * (blocks - my_blocks)
        other_block = (1 - core) * (blocks - my_blocks)
        lanes = my_blocks * block

        def rows(a, start, size):
            return lax.dynamic_slice_in_dim(a, start, size, axis=0)

        def cols(a, start, size):
            return lax.dynamic_slice_in_dim(a, start, size, axis=a.ndim - 1)

        def my_cols(w):
            return cols(w, first_block * block, lanes)

        x_first = [rows(resid_in, (1 - cx) * steps + cy * half + c * quarter, quarter) for c in range(2)]
        far_mine = [px(a) for a in x_first]
        vec = jnp.stack([gain_temporal, gain_mlp, bias_o, bias_d])
        vecs = [vec, pc(vec), px(vec), pd(vec)]
        x_own = rows(resid_in, cx * steps, steps)
        x_near = pc(x_own)
        shares = []
        for w in (w_x, w_y):
            mine, others = my_cols(w), cols(w, other_block * block, lanes)
            shares.append((mine, pc(others), px(mine), pd(others)))
        wo_far = px(w_o)
        bounds = [sum(CHUNKS[:c]) for c in range(len(CHUNKS) + 1)]
        chunk = [slice(lo, hi) for lo, hi in zip(bounds, bounds[1:])]
        gates = [(w, pc(w), px(w)) for part in chunk for w in (w_g[:, part], w_u[:, part])]
        split = SPLIT
        sides = [slice(0, split), slice(split, local_width)]
        d_near = pc(w_d)
        d_far = [px(w_d[:, part]) for part in sides]

        table = jnp.stack([v.astype(f32) for v in vecs], axis=1)
        gain_t, gain_m, b_o, b_d = table[0], table[1], table[2], table[3]

        far_other = [py(a) for a in far_mine]
        far = far_mine + far_other
        diag = [pc(a) for a in far]
        shift = (2 * cy).astype(jnp.int32).reshape(1)
        normed = norm_in(shift, x_own, x_near, far, diag, gain_t)

        u = project(normed, shares[0], my_cols(bias_x), 0, steps)
        rate = -8.0 * jax.nn.softplus(-my_cols(lam_param))
        pos = rows(seg_pos, cx, 1).reshape(steps, 1)
        hidden = recurrence(u, pos, my_cols(conv_w), my_cols(conv_bias), rate,
                            rows(rgate_w, first_block, my_blocks), my_cols(rgate_b),
                            rows(igate_w, first_block, my_blocks), my_cols(igate_b))
        hidden, *wy = tie(hidden, *shares[1])
        given = project(normed, wy, my_cols(bias_y), 1 - core, half, hidden)
        given, hidden = tie(given, hidden)
        got = pc(given)
        kept = project(normed, wy, my_cols(bias_y), core, half, hidden)

        first = core == 0
        mixed_all = jnp.concatenate([jnp.where(first, kept, got), jnp.where(first, got, kept)[:, 2 * lanes - blocks * block:]], axis=1)
        wo = [w_o, pc(w_o)]
        mixed_send = rows(mixed_all, (1 - cy) * quarter, quarter)
        mixed_keep = rows(mixed_all, cy * quarter, quarter)
        cut = quarter // 2
        received = [[None] * 4, [None] * 4]

        def send_part(r, j):
            part = dot(mixed_send[r * cut:(r + 1) * cut], wo[j]).astype(bf16)
            received[r][j] = py(part)
            return part

        ready = [send_part(0, j) for j in (0, 1)]
        mixed_keep, mixed_send, wo_far, *_ = tie(mixed_keep, mixed_send, wo_far, *ready)
        wo += [wo_far, pc(wo_far)]
        for r, j in ((0, 2), (0, 3), (1, 0), (1, 1), (1, 2), (1, 3)):
            send_part(r, j)
        own = [dot(mixed_keep, w) for w in wo]
        my_quarter = core * 2 + cy
        at = jnp.stack([cx * 4 + my_quarter, my_quarter, (my_quarter + 2 * cy) % 4]).astype(jnp.int32)
        m_own, resid = [None] * 2, ()
        for r in range(2):
            resid, m_own[r] = resid_norm(at, r, resid_in, x_near, far, diag, own, received[r], b_o, gain_m, resid)
        m_other = [py(m) for m in m_own]

        def relay(w, far_piece):
            return [w[0], w[1], far_piece, pc(far_piece)]

        def up(m, c, ws, into=None):
            return inner_of(m, ws[0], ws[1], bias_g[chunk[c]], bias_u[chunk[c]], bounds[c], bounds[-1], into)

        def arrive(c, *values):
            *values, far_g, far_u = tie(*values, gates[2 * c][2], gates[2 * c + 1][2])
            return values, (relay(gates[2 * c], far_g), relay(gates[2 * c + 1], far_u))

        m_own, w0 = arrive(0, *m_own)
        inner_own = up(m_own, 0, w0)
        (inner_own,), w1 = arrive(1, inner_own)
        inner_own = up(m_own, 1, w1, inner_own)
        inner_own, *m_other = tie(inner_own, *m_other)
        inner_other = up(m_other, 0, w0)
        inner_other = up(m_other, 1, w1, inner_other)
        for c in (2, 3):
            (inner_other, inner_own), ws = arrive(c, inner_other, inner_own)
            inner_other = up(m_other, c, ws, inner_other)
            inner_own, inner_other = tie(inner_own, inner_other)
            inner_own = up(m_own, c, ws, inner_own)
        (inner_other, inner_own), ws = arrive(4, inner_other, inner_own)
        inner_other = up(m_other, 4, ws, inner_other)

        hops = (lambda a: a, pc, lambda a: over_x(a, 2), lambda a: over_x(a, 3))
        pieces = []
        whole = slice(0, local_width)

        def part(w):
            return dot(inner_other, w).astype(bf16)

        def finish(j, h, mine, down):
            at = (whole,) + tuple(sides)
            return (resid[j][:, at[h]] + (mine + down.astype(f32)) + b_d[j, at[h]]).astype(bf16)

        def hand_on(j, h, out):
            moved = hops[j](out)
            pieces.append((j, (0, 0, split)[h], moved, py(moved)))

        near = [w_d, d_near]
        part1 = part(near[1])
        sum1 = py(part1)
        part0 = part(near[0])
        sum0 = py(part0)
        inner_own, *_ = tie(inner_own, part0, part1)
        inner_own = up(m_own, 4, ws, inner_own)
        out1 = finish(1, 0, dot(inner_own, near[1]), sum1)
        hand_on(1, 0, out1)
        out0 = finish(0, 0, dot(inner_own, near[0]), sum0)
        hand_on(0, 0, out0)
        result = jnp.zeros((tokens, local_width), bf16)
        near_mine = pieces[0][2]
        result = lax.dynamic_update_slice(result, near_mine, (jnp.bitwise_xor(wd, 1) * half + cy * quarter, 0))
        inner_own, inner_other, far_a, *_ = tie(inner_own, inner_other, d_far[0], out0, out1)
        d = [far_a, pc(far_a)]
        parts_a = [part(d[j]) for j in range(2)]
        sums_a = [py(v) for v in parts_a]
        inner_own, *_ = tie(inner_own, *parts_a)
        mine2a = dot(inner_own, d[0])
        mine3a = dot(inner_own, d[1])
        mine_a = tie(mine2a, mine3a)
        out2a = finish(2, 1, mine_a[0], sums_a[0])
        hand_on(2, 1, out2a)
        inner_own, inner_other, far_b, mine3a, _ = tie(inner_own, inner_other, d_far[1], mine_a[1], out2a)
        d = [far_b, pc(far_b)]
        parts_b = [part(d[j]) for j in range(2)]
        sums_b = [py(v) for v in parts_b]
        hand_on(3, 1, finish(3, 1, mine3a, sums_a[1]))
        inner_own, *_ = tie(inner_own, *parts_b)
        mine_b = tie(*[dot(inner_own, w) for w in d])
        for j in range(2):
            hand_on(j + 2, 2, finish(j + 2, 2, mine_b[j], sums_b[j]))
        near_other, own_mine, own_other, _ = tie(pieces[0][3], pieces[1][2], pieces[1][3], mine_b[0])
        pieces[:2] = [(1, 0, near_mine, near_other), (0, 0, own_mine, own_other)]

        for j, col, mine, other in pieces:
            base = jnp.bitwise_xor(wd, j) * half
            for value, row in ((mine, base + cy * quarter), (other, base + (1 - cy) * quarter)):
                if value is not near_mine:
                    result = lax.dynamic_update_slice(result, value, (row, col))
        return result

    return jax.shard_map(local_layer, mesh=mesh, in_specs=specs, out_specs=row_spec, check_vma=False)
```
